256 devices in a mesh: pair: 32 (over z, y), aux: 8 (over x, core).
Axes of the slice: x: 4, y: 4, z: 8, core: 2. Of those that a mesh axis runs over, the one named last changes fastest.
Arguments:
- ints_ac: bfloat16 [768, 512, 4096], P(None, ('pair', 'aux')), may hold values from -0.375 to 0.375
- slot_pair: int32 [768], replicated, may hold values from 0 to 767, each once
- amplitudes: bfloat16 [768, 2, 4096], P(('pair', 'aux')), may hold values from -6 to 6
- ranks: int32 [768], P(('pair', 'aux')), may hold values from 16 to 64
- pair_occ: int32 [768, 2], P(('pair', 'aux')), may hold values from 0 to 47
- pno_energy: float32 [768, 64], P(('pair', 'aux')), may hold values from 0.2 to 3
- occ_energy: float32 [48], replicated, may hold values from -2 to -0.3
Outputs:
- ext_residual: float32 [768, 2, 4096], P(('pair', 'aux'))
- new_amplitudes: bfloat16 [768, 2, 4096], P(('pair', 'aux'))
The draws below stay inside these ranges and needn't reach their ends.
Inputs may be any that keep to these rules, and one draw needn't show every extreme that they name: `slot_pair`: a permutation of the pairs. Entries a >= ranks[s] of a slot's blocks are padding.
All inputs are finite; a program needn't handle non-finite values.
Results may differ from the reference program's by a relative error of at most 0.0039.
Values may be sent and summed in bfloat16 or wider, within the bound.
No kernel may reach another device: no remote copies, remote signals or barrier semaphores. Data moves between devices by JAX's collectives and lax.ppermute only.
A program may use at most 128 MiB of HBM per device.

```python
import jax
import jax.numpy as jnp
from jax import lax

RANK = 64
NAUX = 512
NOCC = 48
PAIRS = 768


def plant(entries, own_key, low, largest):
    longest = entries.shape.index(max(entries.shape))
    spots = []
    for shift in (0, 1):
        where = [jax.random.randint(jax.random.fold_in(own_key, axis), (), 0, length) for axis, length in enumerate(entries.shape)]
        where[longest] = (where[longest] + shift) % entries.shape[longest]
        spots.append(tuple(where))
    return entries.at[spots[0]].set(low).at[spots[1]].set(largest)


def block_scale(rng, dims, pieces, low, top_value):
    level, own = 1.0, jax.random.fold_in(rng, 6)
    for dim, blocks in pieces:
        heights = jnp.exp(jax.random.uniform(jax.random.fold_in(own, dim), (blocks,), jnp.float32, low / len(pieces), top_value / len(pieces)))
        level = level * jnp.repeat(heights, dims[dim] // blocks).reshape([-1 if axis == dim else 1 for axis in range(len(dims))])
    return level


def normal_values(stream_key, extent, spread, most, cuts=(), kind=jnp.bfloat16):
    factor_of = block_scale(stream_key, extent, cuts, -0.22, 0.18) if cuts else 1.0
    array = jax.random.normal(stream_key, extent, jnp.float32) * spread * factor_of
    return jnp.minimum(jnp.maximum(array, -most), most).astype(kind)


def setup_inputs(seed: int = 0) -> dict:
    key_list = jax.random.split(jax.random.key(seed), 8)
    return {
        "ints_ac": normal_values(key_list[0], (PAIRS, NAUX, RANK * RANK), ((NAUX * RANK * RANK) ** -0.25), 0.375, ((1, 256),)),
        "slot_pair": jax.random.permutation(key_list[1], PAIRS).astype(jnp.int32),
        "amplitudes": normal_values(key_list[2], (PAIRS, 2, RANK * RANK), 1.0, 6.0, ((0, 256),)),
        "ranks": plant(jax.random.randint(key_list[3], (PAIRS,), RANK // 4, RANK + 1), jax.random.fold_in(key_list[3], 1), RANK // 4, RANK).astype(jnp.int32),
        "pair_occ": plant(jax.random.randint(key_list[4], (PAIRS, 2), 0, NOCC), jax.random.fold_in(key_list[4], 1), 0, NOCC - 1).astype(jnp.int32),
        "pno_energy": jnp.clip(0.2 + 2.8 * jax.random.uniform(key_list[5], (PAIRS, RANK), jnp.float32) ** block_scale(key_list[5], (PAIRS, RANK), ((0, 256),), -0.2, 0.2), 0.2, 3.0),
        "occ_energy": jnp.clip(jax.random.uniform(key_list[6], (NOCC,), jnp.float32, -2.0, -0.3), -2.0, -0.3),
    }


def reference(ints_ac, slot_pair, amplitudes, ranks, pair_occ, pno_energy, occ_energy):
    positions = jnp.arange(RANK, dtype=jnp.int32)
    masks = (positions[None, :] < ranks[:, None]).astype(jnp.float32)

    def one_slot(slot):
        pair_index = slot_pair[slot].astype(jnp.int32)
        block = lax.dynamic_index_in_dim(ints_ac, pair_index, 0, keepdims=False)
        amps = lax.dynamic_index_in_dim(amplitudes, slot, 0, keepdims=False)
        mask = lax.dynamic_index_in_dim(masks, slot, 0, keepdims=False)
        square = (mask[:, None] * mask[None, :]).reshape(RANK * RANK).astype(jnp.bfloat16)
        masked_b = (block * square).reshape(NAUX, RANK, RANK).astype(jnp.float32)
        masked_t = (amps * square).reshape(2, RANK, RANK).astype(jnp.float32)
        inner = jnp.einsum("pac,kcd->pakd", masked_b, masked_t).astype(jnp.bfloat16).astype(jnp.float32)
        result = jnp.einsum("pakd,pbd->kab", inner, masked_b)
        return result.reshape(2, RANK * RANK)

    ext_residual = lax.map(one_slot, jnp.arange(PAIRS, dtype=jnp.int32))
    occ_pair = occ_energy[pair_occ]
    denom = pno_energy[:, :, None] + pno_energy[:, None, :] - (occ_pair[:, 0] + occ_pair[:, 1])[:, None, None]
    square = masks[:, :, None] * masks[:, None, :]
    masked_t = amplitudes.astype(jnp.float32).reshape(PAIRS, 2, RANK, RANK) * square[:, None]
    updated = (masked_t - ext_residual.reshape(PAIRS, 2, RANK, RANK) / denom[:, None]) * square[:, None]
    new_amplitudes = updated.reshape(PAIRS, 2, RANK * RANK).astype(jnp.bfloat16)
    return ext_residual, new_amplitudes
```

```python
import jax
import jax.numpy as jnp
from jax import lax
from jax.experimental import pallas as pl
from jax.experimental.pallas import tpu as pltpu
from jax.sharding import Mesh, PartitionSpec as P

SIDES = (4, 4, 2)
AXES = ("z", "y", "x", "core")
BF16, F32 = jnp.bfloat16, jnp.float32


def moved(value, axis, step):
    n = lax.axis_size(axis)
    return lax.ppermute(value, axis, [(j, (j + step) % n) for j in range(n)])


class Plan:
    def __init__(self, sizes, local):
        self.nz, self.ny, self.nx, self.nc = sizes
        self.local = local
        self.half = self.nz // 2
        self.batch = self.half * local

    def steps(self, h):
        return (self.ny, self.nx) if h == 0 else (self.nx, self.ny)

    def slot(self, h, s, t, zz, i, meta, core):
        sy, sx = (s, t) if h == 0 else (t, s)
        y = lax.rem(meta[1] - sy + self.ny, self.ny)
        x = lax.rem(meta[2] - sx + self.nx, self.nx)
        z = zz + h * self.half
        return (((z * self.ny + y) * self.nx + x) * self.nc + core) * self.local + i


def collect(plan, rows, slot_pair, meta):
    total = rows.shape[0] // plan.nc
    per_half = total // 2

    def kernel(sp, where, src, out, sem):
        other = 1 - where[3]
        for h in range(2):
            _, inner = plan.steps(h)

            def piece_row(r, carry, h=h, inner=inner):
                s, t = lax.div(r, inner), lax.rem(r, inner)
                for n in range(plan.batch):
                    slot = plan.slot(h, s, t, n // plan.local, n % plan.local, where, other)
                    pltpu.make_async_copy(
                        src.at[sp[slot]], out.at[h * per_half + r * plan.batch + n], sem
                    ).start()
                return carry

            lax.fori_loop(0, per_half // plan.batch, piece_row, 0)
        pltpu.make_async_copy(src.at[pl.ds(0, total)], out, sem).wait()

    return pl.pallas_call(
        kernel,
        grid_spec=pltpu.PrefetchScalarGridSpec(
            num_scalar_prefetch=2,
            grid=(1,),
            in_specs=[pl.BlockSpec(memory_space=pl.ANY)],
            out_specs=pl.BlockSpec(memory_space=pl.ANY),
            scratch_shapes=[pltpu.SemaphoreType.DMA],
        ),
        out_shape=jax.ShapeDtypeStruct((total, *rows.shape[1:]), rows.dtype),
        name="collect",
    )(slot_pair, meta, rows)


def contract(plan, h, s, rows, sibling, amps, slot_pair, meta):
    outer, inner = plan.steps(h)
    width, lanes = rows.shape[1], rows.shape[2]
    side = width // 2
    batch = plan.batch
    first = (h * plan.nx * plan.ny * batch + s * inner * batch) // batch

    def kernel(sp, where, *refs):
        own, (sib, amp, out, wide) = refs[:batch], refs[batch:]
        low = lax.broadcasted_iota(jnp.int32, (side, lanes), 1) < lanes // 2
        zero = jnp.zeros((width, lanes), BF16)
        none = jnp.zeros((side, lanes), F32)
        for n in range(batch):
            base = n * 2 * width
            wide[pl.ds(base, width), :] = own[n][0].astype(F32)
            wide[pl.ds(base + width, width), :] = sib[n].astype(F32)
            parts = [
                wide[pl.ds(base + u * width + p, side, stride=2), :] for u in range(2) for p in range(2)
            ]
            left = jnp.concatenate(parts, axis=0).astype(BF16)
            amp_n = amp[n]
            right = jnp.concatenate(
                [
                    jnp.concatenate([amp_n, zero], axis=1),
                    jnp.concatenate([zero, amp_n], axis=1),
                ],
                axis=0,
            )
            inner_w = jnp.dot(left, right, preferred_element_type=F32).astype(BF16)
            lhs = jnp.concatenate(
                [
                    jnp.concatenate(
                        [
                            inner_w[p * side : (p + 1) * side, u * lanes : (u + 1) * lanes]
                            for p in range(4)
                        ],
                        axis=1,
                    )
                    for u in range(2)
                ],
                axis=0,
            )
            cols = []
            for part in parts:
                turned = pltpu.roll(part, lanes // 2, 1)
                cols.append(
                    jnp.concatenate(
                        [
                            jnp.where(low, part, none),
                            jnp.where(low, turned, none),
                            jnp.where(low, none, turned),
                            jnp.where(low, none, part),
                        ],
                        axis=0,
                    ).astype(BF16)
                )
            rhs = jnp.concatenate(cols, axis=1)
            out[n] = lax.dot_general(
                lhs, rhs, (((1,), (1,)), ((), ())), preferred_element_type=F32
            ).astype(BF16)

    def own_spec(n):
        def where_is(g, sp, where):
            slot = plan.slot(h, s, g, n // plan.local, n % plan.local, where, where[3])
            return sp[slot], 0, 0

        return pl.BlockSpec((1, width, lanes), where_is)

    count = inner * batch
    return pl.pallas_call(
        kernel,
        grid_spec=pltpu.PrefetchScalarGridSpec(
            num_scalar_prefetch=2,
            grid=(inner,),
            in_specs=[own_spec(n) for n in range(batch)]
            + [
                pl.BlockSpec((batch, width, lanes), lambda g, sp, where: (first + g, 0, 0)),
                pl.BlockSpec((batch, width, lanes), lambda g, sp, where: (g, 0, 0)),
            ],
            out_specs=pl.BlockSpec((batch, width, lanes), lambda g, sp, where: (g, 0, 0)),
            scratch_shapes=[pltpu.VMEM((batch * 2 * width, lanes), F32)],
        ),
        out_shape=jax.ShapeDtypeStruct((count, width, lanes), BF16),
        cost_estimate=pl.CostEstimate(
            flops=count * 2 * 2 * (128 * 128 * 256), bytes_accessed=count * 65536, transcendentals=0
        ),
        name="contract",
    )(slot_pair, meta, *([rows] * batch), sibling, amps)


def total_of(values):
    summed = values[0].astype(F32)
    for value in values[1:]:
        summed = summed + value.astype(F32)
    return summed


def body(ints_ac, slot_pair, amplitudes, ranks, pair_occ, pno_energy, occ_energy):
    width = pno_energy.shape[1]
    local = amplitudes.shape[0]
    pairs, held = ints_ac.shape[:2]
    lanes = 2 * width
    plan = Plan(tuple(lax.axis_size(a) for a in AXES), local)
    meta = jnp.stack([lax.axis_index(a) for a in AXES]).astype(jnp.int32)

    positions = jnp.arange(width, dtype=jnp.int32)
    masks = (positions[None, :] < ranks[:, None]).astype(F32)
    square = masks[:, :, None] * masks[:, None, :]
    masked_t = amplitudes.astype(F32).reshape(local, 2, width, width) * square[:, None]

    rows = ints_ac.reshape(pairs, held, width // 2, lanes).transpose(0, 2, 1, 3)
    rows = rows.reshape(pairs, width // 2 * held, lanes)

    mine = masked_t.astype(BF16).transpose(0, 2, 1, 3).reshape(local, width, lanes)
    nz = plan.nz
    column = lax.all_to_all(
        jnp.broadcast_to(mine, (nz, *mine.shape)), "z", split_axis=0, concat_axis=0, tiled=True
    ).reshape(nz * local, width, lanes)

    sent = collect(plan, rows, slot_pair, meta)
    sibling = moved(sent, "core", 1)

    planes = []
    for h in range(2):
        axis = "x" if h == 0 else "y"
        piece = column[h * plan.batch : (h + 1) * plan.batch]
        inner = plan.steps(h)[1]
        planes.append(
            jnp.concatenate([piece] + [moved(piece, axis, t) for t in range(1, inner)], axis=0)
        )
    halves = []
    arrived = {(h, 0): planes[h] for h in range(2)}
    for s in range(1, max(plan.ny, plan.nx)):
        for h in range(2):
            if s < plan.steps(h)[0]:
                arrived[h, s] = moved(planes[h], "y" if h == 0 else "x", s)
    partial = {
        (h, s): contract(plan, h, s, rows, sibling, value, slot_pair, meta)
        for (h, s), value in sorted(arrived.items(), key=lambda item: item[0][::-1])
    }
    for h in range(2):
        outer, inner = plan.steps(h)
        long, short = ("y", "x") if h == 0 else ("x", "y")
        back = [partial[h, 0]] + [moved(partial[h, s], long, -s) for s in range(1, outer)]
        plane = total_of(back).astype(BF16).reshape(inner, plan.batch, width, lanes)
        back = [plane[0]] + [moved(plane[t], short, -t) for t in range(1, inner)]
        halves.append(total_of(back).astype(BF16))
    line = jnp.concatenate(halves, axis=0).reshape(nz, local, width, lanes)
    line = lax.all_to_all(line, "z", split_axis=0, concat_axis=0, tiled=True)
    found = line.astype(F32).sum(axis=0)
    found = found.reshape(local, 2, width // 2, 2, 2, width // 2).transpose(0, 3, 2, 1, 5, 4)
    residual = found.reshape(local, 2, width, width) * square[:, None]

    onehot = (
        pair_occ[:, :, None] == jnp.arange(occ_energy.shape[0], dtype=jnp.int32)[None, None, :]
    ).astype(F32)
    occ_pair = jnp.einsum("jko,o->jk", onehot, occ_energy, precision=lax.Precision.HIGHEST)
    denom = (
        pno_energy[:, :, None]
        + pno_energy[:, None, :]
        - (occ_pair[:, 0] + occ_pair[:, 1])[:, None, None]
    )
    updated = (masked_t - residual / denom[:, None]) * square[:, None]
    return (
        residual.reshape(local, 2, width * width),
        updated.reshape(local, 2, width * width).astype(BF16),
    )


def solution(mesh):
    fine = Mesh(mesh.devices.reshape(-1, *SIDES), AXES)
    placed = (
        P(None, AXES, None),
        P(),
        P(AXES, None, None),
        P(AXES),
        P(AXES, None),
        P(AXES, None),
        P(),
    )
    return jax.shard_map(
        body,
        mesh=fine,
        in_specs=placed,
        out_specs=(P(AXES, None, None), P(AXES, None, None)),
        check_vma=False,
    )
```

```python
import jax
import jax.numpy as jnp
from jax import lax
from jax.experimental import pallas as pl
from jax.experimental.pallas import tpu as pltpu
from jax.sharding import Mesh, PartitionSpec as P


SIDES = (4, 4, 2)
AXES = ("z", "y", "x", "core")
BF16, F32 = jnp.bfloat16, jnp.float32


def moved(value, axis, step):
    n = lax.axis_size(axis)
    return lax.ppermute(value, axis, [(j, (j + step) % n) for j in range(n)])


class Plan:
    def __init__(self, sizes, local):
        self.nz, self.ny, self.nx, self.nc = sizes
        assert self.ny == self.nx
        self.ring = self.nx
        self.local = local
        self.half = self.nz // 2
        self.batch = self.half * local
        self.rows = 2 * self.ring

    def slot(self, s, g, n, meta, core):
        h, t = g // self.ring, g % self.ring
        sy = jnp.where(h == 0, s, t)
        sx = jnp.where(h == 0, t, s)
        y = lax.rem(meta[1] - sy + self.ring, self.ring)
        x = lax.rem(meta[2] - sx + self.ring, self.ring)
        z = n // self.local + h * self.half
        return (((z * self.ny + y) * self.nx + x) * self.nc + core) * self.local + n % self.local


def collect(plan, rows, slot_pair, meta):
    width, lanes = rows.shape[1:]
    batch = plan.batch
    steps = plan.ring * plan.rows

    def kernel(sp, where, *refs):
        out = refs[-1]
        for n in range(batch):
            out[n] = refs[n][0]

    def spec(n):
        def where_is(g, sp, where):
            return sp[plan.slot(g // plan.rows, g % plan.rows, n, where, 1 - where[3])], 0, 0

        return pl.BlockSpec((1, width, lanes), where_is)

    return pl.pallas_call(
        kernel,
        grid_spec=pltpu.PrefetchScalarGridSpec(
            num_scalar_prefetch=2,
            grid=(steps,),
            in_specs=[spec(n) for n in range(batch)],
            out_specs=pl.BlockSpec((batch, width, lanes), lambda g, sp, where: (g, 0, 0)),
        ),
        out_shape=jax.ShapeDtypeStruct((steps * batch, width, lanes), rows.dtype),
        cost_estimate=pl.CostEstimate(
            flops=steps * batch * 10**6, bytes_accessed=steps * batch * 32768, transcendentals=0
        ),
        name="collect",
    )(slot_pair, meta, *([rows] * batch))


def assemble(plan, column, parts):
    batch, ring = plan.batch, plan.ring
    tail = column.shape[1:]

    def kernel(own, *refs):
        got, outs = refs[:-2], refs[-2:]
        for h in range(2):
            outs[h][pl.ds(0, batch)] = own[pl.ds(h * batch, batch)]
            for t in range(1, ring):
                outs[h][pl.ds(t * batch, batch)] = got[h * (ring - 1) + t - 1][...]

    shape = jax.ShapeDtypeStruct((ring * batch, *tail), column.dtype)
    return pl.pallas_call(kernel, out_shape=(shape, shape), name="assemble")(column, *parts)


def contract(plan, s, rows, sibling, amps, slot_pair, meta):
    width, lanes = rows.shape[1], rows.shape[2]
    side = width // 2
    batch, ring = plan.batch, plan.ring

    def kernel(sp, where, *refs):
        own, (sib, amp_0, amp_1, out_0, out_1, token, wide, held) = refs[:batch], refs[batch:]
        g = pl.program_id(0)
        low = lax.broadcasted_iota(jnp.int32, (side, lanes), 1) < lanes // 2
        zero = jnp.zeros((width, lanes), BF16)
        none = jnp.zeros((side, lanes), F32)

        @pl.when(g < ring)
        def _():
            held[...] = amp_0[...]

        @pl.when(g >= ring)
        def _():
            held[...] = amp_1[...]

        for n in range(batch):
            base = n * 2 * width
            wide[pl.ds(base, width), :] = own[n][0].astype(F32)
            wide[pl.ds(base + width, width), :] = sib[n].astype(F32)
            parts = [
                wide[pl.ds(base + u * width + p, side, stride=2), :] for u in range(2) for p in range(2)
            ]
            left = jnp.concatenate(parts, axis=0).astype(BF16)
            amp_n = held[n]
            right = jnp.concatenate(
                [
                    jnp.concatenate([amp_n, zero], axis=1),
                    jnp.concatenate([zero, amp_n], axis=1),
                ],
                axis=0,
            )
            inner_w = jnp.dot(left, right, preferred_element_type=F32).astype(BF16)
            lhs = jnp.concatenate(
                [
                    jnp.concatenate(
                        [
                            inner_w[p * side : (p + 1) * side, u * lanes : (u + 1) * lanes]
                            for p in range(4)
                        ],
                        axis=1,
                    )
                    for u in range(2)
                ],
                axis=0,
            )
            cols = []
            for part in parts:
                turned = pltpu.roll(part, lanes // 2, 1)
                cols.append(
                    jnp.concatenate(
                        [
                            jnp.where(low, part, none),
                            jnp.where(low, turned, none),
                            jnp.where(low, none, turned),
                            jnp.where(low, none, part),
                        ],
                        axis=0,
                    ).astype(BF16)
                )
            rhs = jnp.concatenate(cols, axis=1)
            held[n] = lax.dot_general(
                lhs, rhs, (((1,), (1,)), ((), ())), preferred_element_type=F32
            ).astype(BF16)

        @pl.when(g < ring)
        def _():
            out_0[...] = held[...]

        @pl.when(g >= ring)
        def _():
            out_1[...] = held[...]

        for i in range(4):
            token[i] = where[i]

    def own_spec(n):
        def where_is(g, sp, where):
            return sp[plan.slot(s, g, n, where, where[3])], 0, 0

        return pl.BlockSpec((1, width, lanes), where_is)

    block = (batch, width, lanes)
    first = pl.BlockSpec(block, lambda g, sp, where: (jnp.minimum(g, ring - 1), 0, 0))
    second = pl.BlockSpec(block, lambda g, sp, where: (jnp.maximum(g - ring, 0), 0, 0))
    count = ring * batch
    shape = jax.ShapeDtypeStruct((count, width, lanes), BF16)
    return pl.pallas_call(
        kernel,
        grid_spec=pltpu.PrefetchScalarGridSpec(
            num_scalar_prefetch=2,
            grid=(plan.rows,),
            in_specs=[own_spec(n) for n in range(batch)]
            + [
                pl.BlockSpec(block, lambda g, sp, where: (s * plan.rows + g, 0, 0)),
                first,
                second,
            ],
            out_specs=(first, second, pl.BlockSpec(memory_space=pltpu.SMEM)),
            scratch_shapes=[pltpu.VMEM((batch * 2 * width, lanes), F32), pltpu.VMEM(block, BF16)],
        ),
        out_shape=(shape, shape, jax.ShapeDtypeStruct((4,), jnp.int32)),
        cost_estimate=pl.CostEstimate(
            flops=2 * count * 4 * (128 * 128 * 256),
            bytes_accessed=2 * count * 65536,
            transcendentals=0,
        ),
        name="contract",
    )(slot_pair, meta, *([rows] * batch), sibling, *amps)


def finish(line, amps, denom, square):
    nz, local, width, lanes = line.shape
    side = width // 2

    def kernel(line_ref, amp_ref, den_ref, sq_ref, res_ref, new_ref, wide, part):
        source = lax.broadcasted_iota(jnp.int32, (lanes, lanes), 0)
        target = lax.broadcasted_iota(jnp.int32, (lanes, lanes), 1)
        col = target % width
        for i in range(local):
            total = line_ref[0, i].astype(F32)
            for z in range(1, nz):
                total = total + line_ref[z, i].astype(F32)
            wide[...] = amp_ref[i].astype(F32)
            den, sq = den_ref[i], sq_ref[i]
            for k in range(2):
                value = jnp.zeros((side, lanes), F32)
                for u in range(2):
                    chosen = (target // width == u) & (
                        source == k * width + (col % 2) * side + col // 2
                    )
                    value = value + jnp.dot(
                        total[u * side : (u + 1) * side],
                        chosen.astype(F32),
                        precision=lax.Precision.HIGHEST,
                        preferred_element_type=F32,
                    )
                value = value * sq
                amp = wide[pl.ds(k, side, stride=2), :] * sq
                part[pl.ds(k, side, stride=2), :] = value
                wide[pl.ds(k, side, stride=2), :] = (amp - value / den) * sq
            res_ref[i] = part[...]
            new_ref[i] = wide[...].astype(BF16)

    shape = (local, width, lanes)
    return pl.pallas_call(
        kernel,
        out_shape=(jax.ShapeDtypeStruct(shape, F32), jax.ShapeDtypeStruct(shape, BF16)),
        scratch_shapes=[pltpu.VMEM((width, lanes), F32), pltpu.VMEM((width, lanes), F32)],
        name="finish",
    )(line, amps, denom, square)


def total_of(values):
    summed = values[0].astype(F32)
    for value in values[1:]:
        summed = summed + value.astype(F32)
    return summed


def body(ints_ac, slot_pair, amplitudes, ranks, pair_occ, pno_energy, occ_energy):
    width = pno_energy.shape[1]
    local = amplitudes.shape[0]
    lanes = 2 * width
    plan = Plan(tuple(lax.axis_size(a) for a in AXES), local)
    meta = jnp.stack([lax.axis_index(a) for a in AXES]).astype(jnp.int32)

    positions = jnp.arange(width, dtype=jnp.int32)
    masks = (positions[None, :] < ranks[:, None]).astype(F32)
    square = masks[:, :, None] * masks[:, None, :]
    masked_t = amplitudes.astype(F32).reshape(local, 2, width, width) * square[:, None]

    def paired(value):
        value = value.reshape(value.shape[0], 2, width // 2, lanes).transpose(0, 2, 1, 3)
        return value.reshape(value.shape[0], width, lanes)

    def unpaired(value):
        value = value.reshape(local, width // 2, 2, lanes).transpose(0, 2, 1, 3)
        return value.reshape(local, 2, width * width)

    rows = paired(ints_ac)

    mine = masked_t.astype(BF16).transpose(0, 2, 1, 3).reshape(local, width, lanes)
    nz, ring = plan.nz, plan.ring
    column = lax.all_to_all(
        jnp.broadcast_to(mine, (nz, *mine.shape)), "z", split_axis=0, concat_axis=0, tiled=True
    )
    column = column.reshape(nz * local, width, lanes)

    sent = collect(plan, rows, slot_pair, meta)
    sibling = moved(sent, "core", 1)

    short, long = ("x", "y"), ("y", "x")
    pieces = [column[h * plan.batch : (h + 1) * plan.batch] for h in range(2)]
    parts = [moved(pieces[h], short[h], t) for h in range(2) for t in range(1, ring)]
    planes = assemble(plan, column, parts)
    arrived = [planes] + [
        tuple(moved(planes[h], long[h], s) for h in range(2)) for s in range(1, ring)
    ]
    back = [[], []]
    token = meta
    for s in range(ring):
        *partial, token = contract(plan, s, rows, sibling, arrived[s], slot_pair, token)
        for h in range(2):
            back[h].append(moved(partial[h], long[h], -s) if s else partial[h])
    halves = []
    for h in range(2):
        plane = total_of(back[h]).astype(BF16).reshape(ring, plan.batch, width, lanes)
        last = [plane[0]] + [moved(plane[t], short[h], -t) for t in range(1, ring)]
        halves.append(total_of(last).astype(BF16))
    line = jnp.concatenate(halves, axis=0).reshape(nz, local, width, lanes)
    line = lax.all_to_all(line, "z", split_axis=0, concat_axis=0, tiled=True)

    onehot = (
        pair_occ[:, :, None] == jnp.arange(occ_energy.shape[0], dtype=jnp.int32)[None, None, :]
    ).astype(F32)
    occ_pair = jnp.einsum("jko,o->jk", onehot, occ_energy, precision=lax.Precision.HIGHEST)
    denom = (
        pno_energy[:, :, None]
        + pno_energy[:, None, :]
        - (occ_pair[:, 0] + occ_pair[:, 1])[:, None, None]
    )
    flat = (local, width // 2, lanes)
    residual, updated = finish(line, paired(amplitudes), denom.reshape(flat), square.reshape(flat))
    return unpaired(residual), unpaired(updated)


def solution(mesh):
    fine = Mesh(mesh.devices.reshape(-1, *SIDES), AXES)
    placed = (
        P(None, AXES, None),
        P(),
        P(AXES, None, None),
        P(AXES),
        P(AXES, None),
        P(AXES, None),
        P(),
    )
    return jax.shard_map(
        body,
        mesh=fine,
        in_specs=placed,
        out_specs=(P(AXES, None, None), P(AXES, None, None)),
        check_vma=False,
    )
```

```python
import jax
import jax.numpy as jnp
from jax import lax
from jax.experimental import pallas as pl
from jax.experimental.pallas import tpu as pltpu
from jax.sharding import Mesh, PartitionSpec as P


SIDES = (4, 4, 2)
AXES = ("z", "y", "x", "core")
BF16, F32 = jnp.bfloat16, jnp.float32


def moved(value, axis, step):
    n = lax.axis_size(axis)
    return lax.ppermute(value, axis, [(j, (j + step) % n) for j in range(n)])


class Plan:
    def __init__(self, sizes, local):
        self.nz, self.ny, self.nx, self.nc = sizes
        assert self.ny == self.nx
        self.ring = self.nx
        self.local = local
        self.half = self.nz // 2
        self.batch = self.half * local
        self.rows = self.ring * self.ring

    def bases(self):
        x, y, core = (lax.axis_index(a).astype(jnp.int32) for a in ("x", "y", "core"))
        entry = jnp.arange(4 * self.rows, dtype=jnp.int32)
        h = entry % 2
        t = (entry // 2) % self.ring
        s = (entry // (2 * self.ring)) % self.ring
        side = jnp.where(entry < 2 * self.rows, core, 1 - core)
        py = (y - jnp.where(h == 0, s, t) + self.ring) % self.ring
        px = (x - jnp.where(h == 0, t, s) + self.ring) % self.ring
        return (((h * self.half * self.ny + py) * self.nx + px) * self.nc + side) * self.local

    def offset(self, n):
        return n // self.local * (self.ny * self.nx * self.nc * self.local) + n % self.local

    def row_spec(self, n, first, tail):
        h, n = n // self.batch, n % self.batch

        def where_is(g, sp, base, *_):
            return sp[base[first + 2 * g + h] + self.offset(n)], 0, 0

        return pl.BlockSpec((1, *tail), where_is)


def collect(plan, rows, slot_pair, bases):
    tail = rows.shape[1:]
    both = 2 * plan.batch

    def kernel(sp, base, *refs):
        out = refs[-1]
        for n in range(both):
            out[n] = refs[n][0]

    return pl.pallas_call(
        kernel,
        grid_spec=pltpu.PrefetchScalarGridSpec(
            num_scalar_prefetch=2,
            grid=(plan.rows,),
            in_specs=[plan.row_spec(n, 2 * plan.rows, tail) for n in range(both)],
            out_specs=pl.BlockSpec((both, *tail), lambda g, *_: (g, 0, 0)),
        ),
        out_shape=jax.ShapeDtypeStruct((plan.rows * both, *tail), rows.dtype),
        cost_estimate=pl.CostEstimate(
            flops=plan.rows * both * 10**6,
            bytes_accessed=plan.rows * both * 32768,
            transcendentals=0,
        ),
        name="collect",
    )(slot_pair, bases, *([rows] * both))


def assemble(plan, column, parts):
    batch, ring = plan.batch, plan.ring
    tail = column.shape[1:]

    def kernel(own, *refs):
        got, outs = refs[:-2], refs[-2:]
        for h in range(2):
            outs[h][pl.ds(0, batch)] = own[pl.ds(h * batch, batch)]
            for t in range(1, ring):
                outs[h][pl.ds(t * batch, batch)] = got[h * (ring - 1) + t - 1][...]

    shape = jax.ShapeDtypeStruct((ring * batch, *tail), column.dtype)
    return pl.pallas_call(kernel, out_shape=(shape, shape), name="assemble")(column, *parts)


def contract(plan, s, rows, sibling, amps, slot_pair, bases, token):
    width, lanes = rows.shape[1], rows.shape[2]
    side = width // 2
    batch, ring = plan.batch, plan.ring

    both = 2 * batch

    def kernel(sp, base_of, mark, *refs):
        own, (sib, amp_0, amp_1, out_0, out_1, passed, wide) = refs[:both], refs[both:]
        low = lax.broadcasted_iota(jnp.int32, (side, lanes), 1) < lanes // 2
        zero = jnp.zeros((width, lanes), BF16)
        none = jnp.zeros((side, lanes), F32)

        for n in range(both):
            amp, out = (amp_0, out_0) if n < batch else (amp_1, out_1)
            base = n * 2 * width
            wide[pl.ds(base, width), :] = own[n][0].astype(F32)
            wide[pl.ds(base + width, width), :] = sib[n].astype(F32)
            parts = [
                wide[pl.ds(base + u * width + p, side, stride=2), :] for u in range(2) for p in range(2)
            ]
            left = jnp.concatenate(parts, axis=0).astype(BF16)
            amp_n = amp[n % batch]
            right = jnp.concatenate(
                [
                    jnp.concatenate([amp_n, zero], axis=1),
                    jnp.concatenate([zero, amp_n], axis=1),
                ],
                axis=0,
            )
            inner_w = jnp.dot(left, right, preferred_element_type=F32).astype(BF16)
            lhs = jnp.concatenate(
                [
                    jnp.concatenate(
                        [
                            inner_w[p * side : (p + 1) * side, u * lanes : (u + 1) * lanes]
                            for p in range(4)
                        ],
                        axis=1,
                    )
                    for u in range(2)
                ],
                axis=0,
            )
            cols = []
            for part in parts:
                turned = pltpu.roll(part, lanes // 2, 1)
                cols.append(
                    jnp.concatenate(
                        [
                            jnp.where(low, part, none),
                            jnp.where(low, turned, none),
                            jnp.where(low, none, turned),
                            jnp.where(low, none, part),
                        ],
                        axis=0,
                    ).astype(BF16)
                )
            rhs = jnp.concatenate(cols, axis=1)
            out[n % batch] = lax.dot_general(
                lhs, rhs, (((1,), (1,)), ((), ())), preferred_element_type=F32
            ).astype(BF16)

        passed[0] = mark[0]

    block = (batch, width, lanes)
    own_half = pl.BlockSpec(block, lambda g, *_: (g, 0, 0))
    count = ring * batch
    shape = jax.ShapeDtypeStruct((count, width, lanes), BF16)
    return pl.pallas_call(
        kernel,
        grid_spec=pltpu.PrefetchScalarGridSpec(
            num_scalar_prefetch=3,
            grid=(ring,),
            in_specs=[plan.row_spec(n, 2 * s * ring, (width, lanes)) for n in range(both)]
            + [
                pl.BlockSpec((both, width, lanes), lambda g, *_: (s * ring + g, 0, 0)),
                own_half,
                own_half,
            ],
            out_specs=(own_half, own_half, pl.BlockSpec(memory_space=pltpu.SMEM)),
            scratch_shapes=[pltpu.VMEM((both * 2 * width, lanes), F32)],
        ),
        out_shape=(shape, shape, jax.ShapeDtypeStruct((1,), jnp.int32)),
        cost_estimate=pl.CostEstimate(
            flops=2 * count * 4 * (128 * 128 * 256),
            bytes_accessed=2 * count * 65536,
            transcendentals=0,
        ),
        name="contract",
    )(slot_pair, bases, token, *([rows] * both), sibling, *amps)


def finish(line, amps, denom, square):
    nz, local, width, lanes = line.shape
    side = width // 2

    def kernel(line_ref, amp_ref, den_ref, sq_ref, res_ref, new_ref, wide, part):
        source = lax.broadcasted_iota(jnp.int32, (lanes, lanes), 0)
        target = lax.broadcasted_iota(jnp.int32, (lanes, lanes), 1)
        col = target % width
        for i in range(local):
            total = line_ref[0, i].astype(F32)
            for z in range(1, nz):
                total = total + line_ref[z, i].astype(F32)
            wide[...] = amp_ref[i].astype(F32)
            den, sq = den_ref[i], sq_ref[i]
            for k in range(2):
                value = jnp.zeros((side, lanes), F32)
                for u in range(2):
                    chosen = (target // width == u) & (
                        source == k * width + (col % 2) * side + col // 2
                    )
                    value = value + jnp.dot(
                        total[u * side : (u + 1) * side],
                        chosen.astype(F32),
                        precision=lax.Precision.HIGHEST,
                        preferred_element_type=F32,
                    )
                value = value * sq
                amp = wide[pl.ds(k, side, stride=2), :] * sq
                part[pl.ds(k, side, stride=2), :] = value
                wide[pl.ds(k, side, stride=2), :] = (amp - value / den) * sq
            res_ref[i] = part[...]
            new_ref[i] = wide[...].astype(BF16)

    shape = (local, width, lanes)
    return pl.pallas_call(
        kernel,
        out_shape=(jax.ShapeDtypeStruct(shape, F32), jax.ShapeDtypeStruct(shape, BF16)),
        scratch_shapes=[pltpu.VMEM((width, lanes), F32), pltpu.VMEM((width, lanes), F32)],
        name="finish",
    )(line, amps, denom, square)


def total_of(values):
    summed = values[0].astype(F32)
    for value in values[1:]:
        summed = summed + value.astype(F32)
    return summed


def body(ints_ac, slot_pair, amplitudes, ranks, pair_occ, pno_energy, occ_energy):
    width = pno_energy.shape[1]
    local = amplitudes.shape[0]
    lanes = 2 * width
    plan = Plan(tuple(lax.axis_size(a) for a in AXES), local)
    bases = plan.bases()

    positions = jnp.arange(width, dtype=jnp.int32)
    masks = (positions[None, :] < ranks[:, None]).astype(F32)
    square = masks[:, :, None] * masks[:, None, :]
    masked_t = amplitudes.astype(F32).reshape(local, 2, width, width) * square[:, None]

    def paired(value):
        value = value.reshape(value.shape[0], 2, width // 2, lanes).transpose(0, 2, 1, 3)
        return value.reshape(value.shape[0], width, lanes)

    def unpaired(value):
        value = value.reshape(local, width // 2, 2, lanes).transpose(0, 2, 1, 3)
        return value.reshape(local, 2, width * width)

    rows = paired(ints_ac)

    mine = masked_t.astype(BF16).transpose(0, 2, 1, 3).reshape(local, width, lanes)
    nz, ring = plan.nz, plan.ring
    column = lax.all_to_all(
        jnp.broadcast_to(mine, (nz, *mine.shape)), "z", split_axis=0, concat_axis=0, tiled=True
    )
    column = column.reshape(nz * local, width, lanes)

    sent = collect(plan, rows, slot_pair, bases)
    sibling = moved(sent, "core", 1)

    short, long = ("x", "y"), ("y", "x")
    pieces = [column[h * plan.batch : (h + 1) * plan.batch] for h in range(2)]
    parts = [moved(pieces[h], short[h], t) for h in range(2) for t in range(1, ring)]
    planes = assemble(plan, column, parts)
    arrived = [planes]
    for s in range(1, ring):
        arrived.append(tuple(moved(planes[h], long[h], s) for h in range(2)))
    back = [[], []]
    token = bases[:1]
    for s in range(ring):
        *partial, token = contract(plan, s, rows, sibling, arrived[s], slot_pair, bases, token)
        for h in range(2):
            back[h].append(moved(partial[h], long[h], -s) if s else partial[h])
    halves = []
    for h in range(2):
        plane = total_of(back[h]).astype(BF16).reshape(ring, plan.batch, width, lanes)
        last = [plane[0]] + [moved(plane[t], short[h], -t) for t in range(1, ring)]
        halves.append(total_of(last).astype(BF16))
    line = jnp.concatenate(halves, axis=0).reshape(nz, local, width, lanes)
    line = lax.all_to_all(line, "z", split_axis=0, concat_axis=0, tiled=True)

    onehot = (
        pair_occ[:, :, None] == jnp.arange(occ_energy.shape[0], dtype=jnp.int32)[None, None, :]
    ).astype(F32)
    occ_pair = jnp.einsum("jko,o->jk", onehot, occ_energy, precision=lax.Precision.HIGHEST)
    denom = (
        pno_energy[:, :, None]
        + pno_energy[:, None, :]
        - (occ_pair[:, 0] + occ_pair[:, 1])[:, None, None]
    )
    flat = (local, width // 2, lanes)
    residual, updated = finish(line, paired(amplitudes), denom.reshape(flat), square.reshape(flat))
    return unpaired(residual), unpaired(updated)


def solution(mesh):
    fine = Mesh(mesh.devices.reshape(-1, *SIDES), AXES)
    placed = (
        P(None, AXES, None),
        P(),
        P(AXES, None, None),
        P(AXES),
        P(AXES, None),
        P(AXES, None),
        P(),
    )
    return jax.shard_map(
        body,
        mesh=fine,
        in_specs=placed,
        out_specs=(P(AXES, None, None), P(AXES, None, None)),
        check_vma=False,
    )
```

```python
import jax
import jax.numpy as jnp
from jax import lax
from jax.experimental import pallas as pl
from jax.experimental.pallas import tpu as pltpu
from jax.sharding import Mesh, PartitionSpec as P


SIDES = (4, 4, 2)
AXES = ("z", "y", "x", "core")
BF16, F32 = jnp.bfloat16, jnp.float32


def moved(value, axis, step):
    n = lax.axis_size(axis)
    return lax.ppermute(value, axis, [(j, (j + step) % n) for j in range(n)])


def step_order(ring):
    return sorted(range(ring), key=lambda s: min(s, ring - s))


class Plan:
    def __init__(self, sizes, local):
        self.nz, self.ny, self.nx, self.nc = sizes
        assert self.ny == self.nx
        self.ring = self.nx
        self.local = local
        self.half = self.nz // 2
        self.batch = self.half * local
        self.rows = self.ring * self.ring

    def bases(self):
        x, y, core = (lax.axis_index(a).astype(jnp.int32) for a in ("x", "y", "core"))
        entry = jnp.arange(4 * self.rows, dtype=jnp.int32)
        h = entry % 2
        t = (entry // 2) % self.ring
        s = (entry // (2 * self.ring)) % self.ring
        side = jnp.where(entry < 2 * self.rows, core, 1 - core)
        py = (y - jnp.where(h == 0, s, t) + self.ring) % self.ring
        px = (x - jnp.where(h == 0, t, s) + self.ring) % self.ring
        return (((h * self.half * self.ny + py) * self.nx + px) * self.nc + side) * self.local

    def offset(self, n):
        return n // self.local * (self.ny * self.nx * self.nc * self.local) + n % self.local

    def row_spec(self, n, first, tail):
        h, n = n // self.batch, n % self.batch

        def where_is(g, sp, base, *_):
            return sp[base[first + 2 * g + h] + self.offset(n)], 0, 0

        return pl.BlockSpec((1, *tail), where_is)


def collect(plan, rows, slot_pair, bases):
    tail = rows.shape[1:]
    both = 2 * plan.batch

    def kernel(sp, base, *refs):
        out = refs[-1]
        for n in range(both):
            out[n] = refs[n][0]

    return pl.pallas_call(
        kernel,
        grid_spec=pltpu.PrefetchScalarGridSpec(
            num_scalar_prefetch=2,
            grid=(plan.rows,),
            in_specs=[plan.row_spec(n, 2 * plan.rows, tail) for n in range(both)],
            out_specs=pl.BlockSpec((both, *tail), lambda g, *_: (g, 0, 0)),
        ),
        out_shape=jax.ShapeDtypeStruct((plan.rows * both, *tail), rows.dtype),
        cost_estimate=pl.CostEstimate(
            flops=plan.rows * both * 10**6,
            bytes_accessed=plan.rows * both * 32768,
            transcendentals=0,
        ),
        name="collect",
    )(slot_pair, bases, *([rows] * both))


def assemble(plan, column, parts):
    batch, ring = plan.batch, plan.ring
    tail = column.shape[1:]

    def kernel(own, *refs):
        got, outs = refs[:-2], refs[-2:]
        for h in range(2):
            outs[h][pl.ds(0, batch)] = own[pl.ds(h * batch, batch)]
            for t in range(1, ring):
                outs[h][pl.ds(t * batch, batch)] = got[h * (ring - 1) + t - 1][...]

    shape = jax.ShapeDtypeStruct((ring * batch, *tail), column.dtype)
    return pl.pallas_call(kernel, out_shape=(shape, shape), name="assemble")(column, *parts)


def contract(plan, s, rows, sibling, amps, slot_pair, bases, token):
    width, lanes = rows.shape[1], rows.shape[2]
    side = width // 2
    batch, ring = plan.batch, plan.ring

    both = 2 * batch

    def kernel(sp, base_of, mark, *refs):
        own, (sib, amp_0, amp_1, out_0, out_1, passed, wide) = refs[:both], refs[both:]
        low = lax.broadcasted_iota(jnp.int32, (side, lanes), 1) < lanes // 2
        zero = jnp.zeros((width, lanes), BF16)

        for n in range(both):
            amp, out = (amp_0, out_0) if n < batch else (amp_1, out_1)
            base = n * 2 * width
            wide[pl.ds(base, width), :] = own[n][0].astype(F32)
            wide[pl.ds(base + width, width), :] = sib[n].astype(F32)
            parts = [
                wide[pl.ds(base + u * width + p, side, stride=2), :] for u in range(2) for p in range(2)
            ]
            left = jnp.concatenate(parts, axis=0).astype(BF16)
            amp_n = amp[n % batch]
            right = jnp.concatenate(
                [
                    jnp.concatenate([amp_n, zero], axis=1),
                    jnp.concatenate([zero, amp_n], axis=1),
                ],
                axis=0,
            )
            inner_w = jnp.dot(left, right, preferred_element_type=F32).astype(BF16).astype(F32)
            turns = [pltpu.roll(part, lanes // 2, 1) for part in parts]
            blocks = [
                [inner_w[p * side : (p + 1) * side, u * lanes : (u + 1) * lanes] for u in range(2)]
                for p in range(4)
            ]
            lhs, rhs = [[], []], []
            for p in (0, 2):
                rhs.append(
                    jnp.concatenate(
                        [
                            jnp.where(low, parts[p], turns[p + 1]),
                            jnp.where(low, turns[p], parts[p + 1]),
                        ],
                        axis=0,
                    )
                )
                for u in range(2):
                    even, odd = blocks[p][u], blocks[p + 1][u]
                    lhs[u].append(
                        (
                            jnp.where(low, even, pltpu.roll(odd, lanes // 2, 1)),
                            jnp.where(low, pltpu.roll(even, lanes // 2, 1), odd),
                        )
                    )
            lhs = jnp.concatenate(
                [
                    jnp.concatenate([lhs[u][q][k] for q in range(2)], axis=1)
                    for k in range(2)
                    for u in range(2)
                ],
                axis=0,
            ).astype(BF16)
            rhs = jnp.concatenate(rhs, axis=1).astype(BF16)
            both_k = lax.dot_general(
                lhs, rhs, (((1,), (1,)), ((), ())), preferred_element_type=F32
            )
            out[n % batch] = jnp.concatenate(
                [both_k[:width], both_k[width:]], axis=1
            ).astype(BF16)

        passed[0] = mark[0]

    block = (batch, width, lanes)
    own_half = pl.BlockSpec(block, lambda g, *_: (g, 0, 0))
    count = ring * batch
    shape = jax.ShapeDtypeStruct((count, width, lanes), BF16)
    return pl.pallas_call(
        kernel,
        grid_spec=pltpu.PrefetchScalarGridSpec(
            num_scalar_prefetch=3,
            grid=(ring,),
            in_specs=[plan.row_spec(n, 2 * s * ring, (width, lanes)) for n in range(both)]
            + [
                pl.BlockSpec((both, width, lanes), lambda g, *_: (s * ring + g, 0, 0)),
                own_half,
                own_half,
            ],
            out_specs=(own_half, own_half, pl.BlockSpec(memory_space=pltpu.SMEM)),
            scratch_shapes=[pltpu.VMEM((both * 2 * width, lanes), F32)],
        ),
        out_shape=(shape, shape, jax.ShapeDtypeStruct((1,), jnp.int32)),
        cost_estimate=pl.CostEstimate(
            flops=2 * count * 4 * (128 * 128 * 256),
            bytes_accessed=2 * count * 65536,
            transcendentals=0,
        ),
        name="contract",
    )(slot_pair, bases, token, *([rows] * both), sibling, *amps)


def finish(line, amps, denom, square):
    nz, local, width, lanes = line.shape
    side = width // 2

    def kernel(line_ref, amp_ref, den_ref, sq_ref, res_ref, new_ref, wide, part):
        source = lax.broadcasted_iota(jnp.int32, (lanes, lanes), 0)
        target = lax.broadcasted_iota(jnp.int32, (lanes, lanes), 1)
        col = target % width
        for i in range(local):
            total = line_ref[0, i].astype(F32)
            for z in range(1, nz):
                total = total + line_ref[z, i].astype(F32)
            wide[...] = amp_ref[i].astype(F32)
            den, sq = den_ref[i], sq_ref[i]
            for k in range(2):
                value = jnp.zeros((side, lanes), F32)
                for u in range(2):
                    chosen = (target // width == u) & (
                        source == k * width + (col % 2) * side + col // 2
                    )
                    value = value + jnp.dot(
                        total[u * side : (u + 1) * side],
                        chosen.astype(F32),
                        precision=lax.Precision.HIGHEST,
                        preferred_element_type=F32,
                    )
                value = value * sq
                amp = wide[pl.ds(k, side, stride=2), :] * sq
                part[pl.ds(k, side, stride=2), :] = value
                wide[pl.ds(k, side, stride=2), :] = (amp - value / den) * sq
            res_ref[i] = part[...]
            new_ref[i] = wide[...].astype(BF16)

    shape = (local, width, lanes)
    return pl.pallas_call(
        kernel,
        out_shape=(jax.ShapeDtypeStruct(shape, F32), jax.ShapeDtypeStruct(shape, BF16)),
        scratch_shapes=[pltpu.VMEM((width, lanes), F32), pltpu.VMEM((width, lanes), F32)],
        name="finish",
    )(line, amps, denom, square)


def total_of(values):
    summed = values[0].astype(F32)
    for value in values[1:]:
        summed = summed + value.astype(F32)
    return summed


def body(ints_ac, slot_pair, amplitudes, ranks, pair_occ, pno_energy, occ_energy):
    width = pno_energy.shape[1]
    local = amplitudes.shape[0]
    lanes = 2 * width
    plan = Plan(tuple(lax.axis_size(a) for a in AXES), local)
    bases = plan.bases()

    positions = jnp.arange(width, dtype=jnp.int32)
    masks = (positions[None, :] < ranks[:, None]).astype(F32)
    square = masks[:, :, None] * masks[:, None, :]
    masked_t = amplitudes.astype(F32).reshape(local, 2, width, width) * square[:, None]

    def paired(value):
        value = value.reshape(value.shape[0], 2, width // 2, lanes).transpose(0, 2, 1, 3)
        return value.reshape(value.shape[0], width, lanes)

    def unpaired(value):
        value = value.reshape(local, width // 2, 2, lanes).transpose(0, 2, 1, 3)
        return value.reshape(local, 2, width * width)

    rows = paired(ints_ac)

    mine = masked_t.astype(BF16).transpose(0, 2, 1, 3).reshape(local, width, lanes)
    nz, ring = plan.nz, plan.ring
    column = lax.all_to_all(
        jnp.broadcast_to(mine, (nz, *mine.shape)), "z", split_axis=0, concat_axis=0, tiled=True
    )
    column = column.reshape(nz * local, width, lanes)

    sent = collect(plan, rows, slot_pair, bases)
    sibling = moved(sent, "core", 1)

    short, long = ("x", "y"), ("y", "x")
    pieces = [column[h * plan.batch : (h + 1) * plan.batch] for h in range(2)]
    parts = [moved(pieces[h], short[h], t) for h in range(2) for t in range(1, ring)]
    planes = assemble(plan, column, parts)
    arrived = [planes]
    for s in range(1, ring):
        arrived.append(tuple(moved(planes[h], long[h], s) for h in range(2)))
    back = [[], []]
    token = bases[:1]
    for s in step_order(ring):
        *partial, token = contract(plan, s, rows, sibling, arrived[s], slot_pair, bases, token)
        for h in range(2):
            back[h].append(moved(partial[h], long[h], -s) if s else partial[h])
    halves = []
    for h in range(2):
        plane = total_of(back[h]).astype(BF16).reshape(ring, plan.batch, width, lanes)
        last = [plane[0]] + [moved(plane[t], short[h], -t) for t in range(1, ring)]
        halves.append(total_of(last).astype(BF16))
    line = jnp.concatenate(halves, axis=0).reshape(nz, local, width, lanes)
    line = lax.all_to_all(line, "z", split_axis=0, concat_axis=0, tiled=True)

    onehot = (
        pair_occ[:, :, None] == jnp.arange(occ_energy.shape[0], dtype=jnp.int32)[None, None, :]
    ).astype(F32)
    occ_pair = jnp.einsum("jko,o->jk", onehot, occ_energy, precision=lax.Precision.HIGHEST)
    denom = (
        pno_energy[:, :, None]
        + pno_energy[:, None, :]
        - (occ_pair[:, 0] + occ_pair[:, 1])[:, None, None]
    )
    flat = (local, width // 2, lanes)
    residual, updated = finish(line, paired(amplitudes), denom.reshape(flat), square.reshape(flat))
    return unpaired(residual), unpaired(updated)


def solution(mesh):
    fine = Mesh(mesh.devices.reshape(-1, *SIDES), AXES)
    placed = (
        P(None, AXES, None),
        P(),
        P(AXES, None, None),
        P(AXES),
        P(AXES, None),
        P(AXES, None),
        P(),
    )
    return jax.shard_map(
        body,
        mesh=fine,
        in_specs=placed,
        out_specs=(P(AXES, None, None), P(AXES, None, None)),
        check_vma=False,
    )
```
